128 devices in a mesh: dp: 4 (over x), expert: 32 (over y, z, core).
Axes of the slice: x: 4, y: 4, z: 4, core: 2. Of those that a mesh axis runs over, the one named last changes fastest.
Arguments:
- hidden: bfloat16 [196608, 1024], P(('dp', 'expert')), may hold values from -24 to 24
- dout: bfloat16 [196608, 7168], P(('dp', 'expert')), may hold values from -1536 to 1536
- counts: int32 [128, 256], P(('dp', 'expert')), may hold values from 1 to 1536, as said below
- bucket_expert: int32 [1], replicated, may hold values from 0 to 255
- param: float32 [1024, 7168], P(('dp', 'expert')), may hold values from -0.1875 to 0.1875
- momentum: float32 [1024, 7168], P(('dp', 'expert')), may hold values from -3 to 3
Outputs:
- new_param: float32 [1024, 7168], P(('dp', 'expert'))
- new_momentum: float32 [1024, 7168], P(('dp', 'expert'))
- direction: float32 [1024, 7168], P(('dp', 'expert'))
The draws below stay inside these ranges and needn't reach their ends.
Inputs may be any that keep to these rules, and one draw needn't show every extreme that they name: `counts`: row k is device k's count; its rows k * 1536 + t with t below the count are live. For every expert some device has exactly 1536.
All inputs are finite; a program needn't handle non-finite values.
Results may differ from the reference program's by a relative error of at most 0.0003.
Values sent between devices are 32-bit elements; how exact they have to be, the bound alone decides.
A program may use at most 128 MiB of HBM per device.

```python
import jax
import jax.numpy as jnp
from jax import lax

FW = 1024
DW = 7168
NE = 256
TOK_DEV = 1536
TOKENS = 196608
N_DP = 4
N_EXPERT = 32


def draw_counts(key, part):
    ndevices = N_DP * N_EXPERT
    first_key, second_key = jax.random.split(jax.random.fold_in(key, 17))
    device = lax.broadcasted_iota(jnp.int32, (ndevices, NE), 0)
    ceiling = TOK_DEV * (ndevices + 2 * device) // (3 * ndevices)
    drawn = jax.random.randint(first_key, (ndevices, NE), 0, 1 << 20) % (ceiling + 1)
    drawn = jnp.maximum(drawn, 1)
    busiest = jax.random.randint(second_key, (1, NE), 0, ndevices)
    return jnp.where(device == busiest, TOK_DEV, drawn).astype(jnp.int32)


def with_spikes(values, key, source, target, blocks, factor):
    owner, partner = [(jnp.arange(values.shape[dim]) // (values.shape[dim] // blocks)).reshape([-1 if axis == dim else 1 for axis in range(values.ndim)]) for dim in (source, target)]
    chosen = jax.random.permutation(key, blocks)[partner]
    strong = (owner == chosen) | (owner == (partner + blocks // 2) % blocks)
    return jnp.where(strong, factor * values, values)


def block_levels(own_key, dims, shards, low, high):
    def one(dim, shards_of):
        heights = jax.random.uniform(jax.random.fold_in(jax.random.fold_in(own_key, 6), dim), (shards_of,), jnp.float32, low / len(shards), high / len(shards))
        return jnp.repeat(jnp.exp(heights), dims[dim] // shards_of).reshape((-1,) + (1,) * (len(dims) - dim - 1))

    level = one(*shards[0])
    for cut in shards[1:]:
        level = level * one(*cut)
    return level


def gaussian(key, extent, spread, most, shards=(), held_as=jnp.bfloat16):
    loudness = block_levels(key, extent, shards, -0.22, 0.18) if shards else 1.0
    values = jax.random.normal(key, extent, jnp.float32) * spread * loudness
    return jnp.minimum(jnp.maximum(values, -most), most).astype(held_as)


def bell_draw_with(own_key, shape, width, most, cuts, heavy, kind=jnp.bfloat16):
    entries = width * jax.random.normal(own_key, shape, jnp.float32)
    if cuts:
        entries = entries * block_levels(own_key, shape, cuts, -0.22, 0.18)
    return jnp.clip(with_spikes(entries, jax.random.fold_in(own_key, 3), *heavy), -most, most).astype(kind)


def setup_inputs(seed: int = 0) -> dict:
    arg_keys = jax.random.split(jax.random.key(seed), 7)
    hidden = bell_draw_with(arg_keys[0], (TOKENS, FW), 1.0, 24.0, ((0, 128),), (0, 1, 128, 5.5))
    dout = gaussian(arg_keys[1], (TOKENS, DW), (TOK_DEV // 6), 1536.0, ((0, 128),))
    counts = draw_counts(jax.random.fold_in(arg_keys[6], 71), 0)
    bucket_expert = jax.random.randint(arg_keys[3], (1,), 0, NE).astype(jnp.int32)
    param = gaussian(arg_keys[4], (FW, DW), FW ** -0.5, 0.1875, ((0, 128),), jnp.float32)
    momentum = gaussian(arg_keys[5], (FW, DW), 0.5, 3.0, ((0, 128),), jnp.float32)
    return dict(hidden=hidden, dout=dout, counts=counts, bucket_expert=bucket_expert, param=param, momentum=momentum)


first_beta = 0.9
second_beta = 0.99
decay_rate = 0.1
learn_rate = 0.001
soft_width = 0.05


def reference(hidden, dout, counts, bucket_expert, param, momentum):
    catalog = jnp.arange(counts.shape[1], dtype=jnp.int32)[None, :]
    local = jnp.sum(jnp.where(catalog == bucket_expert[0], counts, 0), axis=1).astype(jnp.int32)
    total = jnp.sum(local).astype(jnp.float32)
    position = jnp.arange(hidden.shape[0], dtype=jnp.int32) % TOK_DEV
    limit = jnp.repeat(local, TOK_DEV, total_repeat_length=hidden.shape[0])
    masked = jnp.where((position < limit)[:, None], hidden, jnp.zeros_like(hidden))
    summed = lax.dot_general(masked, dout, (((0,), (0,)), ((), ())), preferred_element_type=jnp.float32)
    grad = summed / total
    blend = first_beta * momentum + (1.0 - first_beta) * grad
    direction = jnp.tanh(blend / soft_width) + decay_rate * param
    new_param = param - learn_rate * direction
    new_momentum = second_beta * momentum + (1.0 - second_beta) * grad
    return new_param, new_momentum, direction
```

```python
import jax
import jax.numpy as jnp
from jax import lax
from jax.experimental import pallas as pl
from jax.experimental.pallas import tpu as pltpu
from jax.sharding import Mesh
from jax.sharding import PartitionSpec as P

AXES = ("x", "y", "z", "c")
MESH = pl.DeviceIdType.MESH

first_beta = 0.9
second_beta = 0.99
decay_rate = 0.1
learn_rate = 0.001
soft_width = 0.05

ROWS = 1536
WIDTH = 1024
PAIR = 256
PAIRS = 28
THEIR_SLOTS = 6
DOUT_SLOTS = 4
HIDDEN_CHUNKS = 4

GROUPS = ((1, 1, 1), (2, 2, 2), (2, 2, 2), (2, 2, 2), (2, 1, 1), (1, 1, 1))
ORDERS = ((0, 2, 1), (1, 0, 2), (2, 1, 0))


def plan():
    groups = []
    pair = 0
    number = 0
    for sizes in GROUPS:
        units = []
        for colour, size in enumerate(sizes):
            if size:
                units.append((number, ORDERS[colour], pair, size))
                number += 1
                pair += size
        groups.append(units)
    assert pair == PAIRS
    return groups, number


PLAN, UNITS = plan()


def kernel(
    counts_ref,
    bucket_ref,
    hidden_ref,
    dout_ref,
    sum_ref,
    total_ref,
    hidden_buf,
    lhs,
    dout_buf,
    acc,
    crossed,
    first_in,
    second_in,
    third_in,
    tally,
    tally_in,
    hidden_sem,
    dout_sem,
    cross_send,
    cross_recv,
    first_send,
    first_hop,
    first_rest,
    second_send,
    second_hop,
    second_rest,
    third_send,
    third_recv,
    tally_send,
    tally_recv,
):
    me = tuple(lax.axis_index(axis) for axis in AXES)
    core = me[3]

    def shifted(dim, by):
        return lax.rem(me[dim] + by, 4)

    def peer(dim, by):
        return tuple(shifted(dim, by) if axis == dim else me[axis] for axis in range(4))

    partner = (me[0], me[1], me[2], 1 - core)

    barrier = pltpu.get_barrier_semaphore()
    pl.semaphore_signal(barrier, inc=1, device_id=partner, device_id_type=MESH)
    for dim in range(3):
        for by in (1, 2, 3):
            pl.semaphore_signal(barrier, inc=1, device_id=peer(dim, by), device_id_type=MESH)

    chunk = ROWS // HIDDEN_CHUNKS

    def hidden_copy(part):
        rows = pl.ds(part * chunk, chunk)
        return pltpu.make_async_copy(hidden_ref.at[rows], hidden_buf.at[rows], hidden_sem.at[part])

    def dout_copy(pair):
        slot = lax.rem(pair, DOUT_SLOTS)
        columns = pl.ds(pl.multiple_of(pair * PAIR, PAIR), PAIR)
        return pltpu.make_async_copy(dout_ref.at[:, columns], dout_buf.at[slot], dout_sem.at[slot])

    for part in range(HIDDEN_CHUNKS):
        hidden_copy(part).start()
    for pair in range(DOUT_SLOTS - 1):
        dout_copy(pair).start()

    own_count = counts_ref[0, bucket_ref[0]]

    for part in range(HIDDEN_CHUNKS):
        hidden_copy(part).wait()

        def turn(step, carry, part=part):
            row = pl.multiple_of(part * chunk + step * 128, 128)
            position = lax.broadcasted_iota(jnp.int32, (128, WIDTH), 0) + row
            live = jnp.where(position < own_count, 1.0, 0.0).astype(jnp.bfloat16)
            masked = hidden_buf[pl.ds(row, 128), :] * live
            lhs[:, pl.ds(row, 128)] = masked.T
            return carry

        lax.fori_loop(0, chunk // 128, turn, 0)

    tally[0] = jnp.full((8, 128), own_count, jnp.int32).astype(jnp.float32)

    pl.semaphore_wait(barrier, 10)

    def remote(source, target, send, recv, device):
        return pltpu.make_async_remote_copy(
            src_ref=source,
            dst_ref=target,
            send_sem=send,
            recv_sem=recv,
            device_id=device,
            device_id_type=MESH,
        )

    def arrived(target, recv):
        remote(target, target, recv, recv, partner).wait_recv()

    def left(source, send):
        remote(source, source, send, send, partner).wait_send()

    def cross_copy(pair):
        slot = lax.rem(pair, THEIR_SLOTS)
        return remote(acc.at[slot], crossed.at[pair], cross_send.at[slot], cross_recv.at[pair], partner)

    def product(pair, carry):
        slot = lax.rem(pair, DOUT_SLOTS)
        dout_copy(pair).wait()

        @pl.when(pair + (DOUT_SLOTS - 1) < PAIRS)
        def _():
            dout_copy(pair + (DOUT_SLOTS - 1)).start()

        @pl.when(pair >= THEIR_SLOTS)
        def _():
            left(acc.at[lax.rem(pair, THEIR_SLOTS)], cross_send.at[lax.rem(pair, THEIR_SLOTS)])

        theirs = lax.rem(pair, THEIR_SLOTS)
        mine = THEIR_SLOTS + pair
        place_0 = core * theirs + (1 - core) * mine
        place_1 = core * mine + (1 - core) * theirs
        for half in range(2):
            rows = pl.ds(half * (WIDTH // 2), WIDTH // 2)
            value = jnp.dot(lhs[rows, :], dout_buf[slot], preferred_element_type=jnp.float32)
            value = value.reshape(2, 4, 4, 2, 8, PAIR)
            acc[place_0, 2 * half : 2 * half + 2] = value[:, :, :, 0]
            acc[place_1, 2 * half : 2 * half + 2] = value[:, :, :, 1]
        cross_copy(pair).start()
        return carry

    def products(group):
        lax.fori_loop(group[0][2], group[-1][2] + group[-1][3], product, 0)

    def at(where):
        return tuple(where.get(dim, slice(None)) for dim in range(3))

    def half_of(side):
        return pl.ds(2 * side, 2)

    def first_region(order, place, side):
        cut = min(order[1], order[2])
        return at({order[0]: place, cut: half_of(side)})

    def second_region(order, place, side):
        return at({order[0]: me[order[0]], order[1]: place, order[2]: half_of(side)})

    def third_region(order, place):
        return at({order[0]: me[order[0]], order[1]: me[order[1]], order[2]: place})

    def gather(pair, size, region, terms):
        for step in range(size):
            spot = (THEIR_SLOTS + pair + step,) + region
            value = acc[spot]
            for ref, index in terms:
                value = value + ref[(pair + step,) + index]
            acc[spot] = value

    def first_copy(unit, kind):
        number, order, pair, size = unit
        by = (2, 2, 1, 3, 1, 3)[kind]
        side = (0, 1, 1, 0, 0, 1)[kind]
        region = first_region(order, shifted(order[0], by), side)
        recv = first_hop if kind < 2 else first_rest
        copy = remote(
            acc.at[(pl.ds(THEIR_SLOTS + pair, size),) + region],
            first_in.at[pl.ds(pair, size), kind],
            first_send.at[number],
            recv.at[number],
            peer(order[0], (1, 3)[kind % 2]),
        )
        return copy, region

    def second_copy(unit, kind):
        number, order, pair, size = unit
        by = (2, 2, 1, 3, 1, 3)[kind]
        side = (0, 1, 1, 0, 0, 1)[kind]
        region = second_region(order, shifted(order[1], by), side)
        recv = second_hop if kind < 2 else second_rest
        copy = remote(
            acc.at[(pl.ds(THEIR_SLOTS + pair, size),) + region],
            second_in.at[pl.ds(pair, size), kind],
            second_send.at[number],
            recv.at[number],
            peer(order[1], (1, 3)[kind % 2]),
        )
        return copy, region

    def third_copy(unit, by):
        number, order, pair, size = unit
        return remote(
            acc.at[(pl.ds(THEIR_SLOTS + pair, size),) + third_region(order, shifted(order[2], by))],
            third_in.at[pl.ds(pair, size), by - 1],
            third_send.at[number],
            third_recv.at[number],
            peer(order[2], by),
        )

    def stage_1(unit):
        number, order, pair, size = unit
        for step in range(size):
            arrived(crossed.at[pair + step], cross_recv.at[pair + step])
        for kind in range(4):
            copy, region = first_copy(unit, kind)
            gather(pair, size, region, ((crossed, region),))
            copy.start()

    def stage_2(unit):
        number, order, pair, size = unit
        arrived(first_in.at[pl.ds(pair, size), pl.ds(0, 2)], first_hop.at[number])
        for kind in (4, 5):
            copy, region = first_copy(unit, kind)
            gather(pair, size, region, ((crossed, region), (first_in, (kind - 4,))))
            copy.start()

    def stage_3(unit):
        number, order, pair, size = unit
        arrived(first_in.at[pl.ds(pair, size), pl.ds(2, 4)], first_rest.at[number])
        left(first_in.at[pl.ds(pair, size)], first_send.at[number])
        for side, (up, down) in enumerate(((4, 3), (2, 5))):
            region = first_region(order, me[order[0]], side)
            gather(pair, size, region, ((crossed, region), (first_in, (up,)), (first_in, (down,))))
        for kind in range(4):
            second_copy(unit, kind)[0].start()

    def stage_4(unit):
        number, order, pair, size = unit
        arrived(second_in.at[pl.ds(pair, size), pl.ds(0, 2)], second_hop.at[number])
        for kind in (4, 5):
            copy, region = second_copy(unit, kind)
            gather(pair, size, region, ((second_in, (kind - 4,)),))
            copy.start()

    def stage_5(unit):
        number, order, pair, size = unit
        arrived(second_in.at[pl.ds(pair, size), pl.ds(2, 4)], second_rest.at[number])
        left(second_in.at[pl.ds(pair, size)], second_send.at[number])
        for side, (up, down) in enumerate(((4, 3), (2, 5))):
            region = second_region(order, me[order[1]], side)
            gather(pair, size, region, ((second_in, (up,)), (second_in, (down,))))
        for by in (1, 2, 3):
            third_copy(unit, by).start()

    def stage_6(unit):
        number, order, pair, size = unit
        arrived(third_in.at[pl.ds(pair, size)], third_recv.at[number])
        left(third_in.at[pl.ds(pair, size)], third_send.at[number])
        region = third_region(order, me[order[2]])
        for step in range(size):
            value = acc[(THEIR_SLOTS + pair + step,) + region]
            for by in range(3):
                value = value + third_in[pair + step, by]
            sum_ref[:, pl.ds((pair + step) * PAIR, PAIR)] = value

    def tally_start(level):
        if level == 0:
            remote(tally.at[0], tally_in.at[0, 0], tally_send.at[0], tally_recv.at[0], partner).start()
        else:
            for by in (1, 2, 3):
                remote(
                    tally.at[level],
                    tally_in.at[level, by - 1],
                    tally_send.at[level],
                    tally_recv.at[level],
                    peer(level - 1, by),
                ).start()

    def tally_end(level):
        number = 1 if level == 0 else 3
        arrived(tally_in.at[level, pl.ds(0, number)], tally_recv.at[level])
        left(tally_in.at[level, pl.ds(0, number)], tally_send.at[level])
        value = tally[level]
        for by in range(number):
            value = value + tally_in[level, by]
        tally[level + 1] = value

    stages = (stage_1, stage_2, stage_3, stage_4, stage_5, stage_6)
    tally_start(0)
    products(PLAN[0])
    for step in range(len(PLAN) + len(stages) - 1):
        if step + 1 < len(PLAN):
            products(PLAN[step + 1])
        for lag, stage in enumerate(stages):
            if 0 <= step - lag < len(PLAN):
                for unit in PLAN[step - lag]:
                    stage(unit)
        if step < 4:
            tally_end(step)
            if step < 3:
                tally_start(step + 1)
    total_ref[...] = tally[4]
    for slot in range(THEIR_SLOTS):
        left(acc.at[slot], cross_send.at[slot])


def reduced(counts, bucket_expert, hidden, dout):
    f32 = jnp.float32
    dma = pltpu.SemaphoreType.DMA
    vmem = pl.BlockSpec(memory_space=pltpu.VMEM)
    smem = pl.BlockSpec(memory_space=pltpu.SMEM)
    away = pl.BlockSpec(memory_space=pl.ANY)
    return pl.pallas_call(
        kernel,
        out_shape=(
            jax.ShapeDtypeStruct((8, PAIR * PAIRS), f32),
            jax.ShapeDtypeStruct((8, 128), f32),
        ),
        in_specs=[smem, smem, away, away],
        out_specs=(vmem, vmem),
        scratch_shapes=[
            pltpu.VMEM((ROWS, WIDTH), jnp.bfloat16),
            pltpu.VMEM((WIDTH, ROWS), jnp.bfloat16),
            pltpu.VMEM((DOUT_SLOTS, ROWS, PAIR), jnp.bfloat16),
            pltpu.VMEM((THEIR_SLOTS + PAIRS, 4, 4, 4, 8, PAIR), f32),
            pltpu.VMEM((PAIRS, 4, 4, 4, 8, PAIR), f32),
            pltpu.VMEM((PAIRS, 6, 2, 4, 8, PAIR), f32),
            pltpu.VMEM((PAIRS, 6, 2, 8, PAIR), f32),
            pltpu.VMEM((PAIRS, 3, 8, PAIR), f32),
            pltpu.VMEM((5, 8, 128), f32),
            pltpu.VMEM((4, 3, 8, 128), f32),
            dma((HIDDEN_CHUNKS,)),
            dma((DOUT_SLOTS,)),
            dma((THEIR_SLOTS,)),
            dma((PAIRS,)),
            dma((UNITS,)),
            dma((UNITS,)),
            dma((UNITS,)),
            dma((UNITS,)),
            dma((UNITS,)),
            dma((UNITS,)),
            dma((UNITS,)),
            dma((UNITS,)),
            dma((4,)),
            dma((4,)),
        ],
        compiler_params=pltpu.CompilerParams(
            collective_id=0, has_side_effects=True, vmem_limit_bytes=67043328
        ),
    )(counts, bucket_expert, hidden, dout)


def body(hidden, dout, counts, bucket_expert, param, momentum):
    summed, total = reduced(counts, bucket_expert, hidden, dout)
    grad = summed / total[0, 0]
    blend = first_beta * momentum + (1.0 - first_beta) * grad
    direction = jnp.tanh(blend / soft_width) + decay_rate * param
    new_param = param - learn_rate * direction
    new_momentum = second_beta * momentum + (1.0 - second_beta) * grad
    return (new_param, new_momentum, direction)


def solution(mesh):
    split = Mesh(mesh.devices.reshape(4, 4, 4, 2), AXES)
    rows = P(AXES, None)
    return jax.shard_map(
        body,
        mesh=split,
        in_specs=(rows, rows, rows, P(), rows, rows),
        out_specs=(rows, rows, rows),
        check_vma=False,
    )
```

```python
import jax
import jax.numpy as jnp
from jax import lax
from jax.experimental import pallas as pl
from jax.experimental.pallas import tpu as pltpu
from jax.sharding import Mesh
from jax.sharding import PartitionSpec as P

AXES = ("x", "y", "z", "c")
MESH = pl.DeviceIdType.MESH

first_beta = 0.9
second_beta = 0.99
decay_rate = 0.1
learn_rate = 0.001
soft_width = 0.05

ROWS = 1536
WIDTH = 1024
PAIR = 256
PAIRS = 28
THEIR_SLOTS = 6
DOUT_SLOTS = 4
HIDDEN_CHUNKS = 6

SIZES = (
    (1, 1, 1, 1, 1, 1, 1, 1, 1, 1),
    (1, 1, 1, 1, 1, 1, 1, 1, 1),
    (1, 1, 1, 1, 1, 1, 1, 1, 1),
)
ORDERS = ((0, 2, 1), (1, 0, 2), (2, 1, 0))
SWAPPED = ((3, 6), (2, 4, 6), ())
LEAD = 3
BLOCK = 4
TALLY_AFTER = (3, 9, 15, 21)


def make_units():
    units = []
    pair = 0
    for turn in range(max(len(sizes) for sizes in SIZES)):
        for colour, sizes in enumerate(SIZES):
            if turn < len(sizes):
                order = ORDERS[colour]
                if turn in SWAPPED[colour]:
                    order = (order[0], order[2], order[1])
                units.append((len(units), order, pair, sizes[turn]))
                pair += sizes[turn]
    assert pair == PAIRS
    return units


def list_schedule(units):
    product_us, cross_us, latency_us, piece_us = 1.03, 0.85, 2.0, 1.405
    free = {(dim, way): 0.0 for dim in range(3) for way in range(2)}
    level = [0] * len(units)
    ready = [None] * len(units)
    rest = [0.0] * len(units)
    crossed = []
    cross_free = 0.0
    now = 0.0
    order = []

    def send(dim, way, duration):
        free[dim, way] = max(free[dim, way], now) + duration
        return free[dim, way] + latency_us

    while min(level) < 6:
        for number, (_, _, pair, size) in enumerate(units):
            if level[number] == 0 and pair + size <= len(crossed):
                ready[number] = max(crossed[pair : pair + size])
        waiting = [n for n in range(len(units)) if level[n] < 6 and ready[n] is not None]
        first = min(waiting, key=lambda n: (ready[n], n), default=None)
        if len(crossed) < PAIRS and (len(crossed) < LEAD or first is None or ready[first] > now):
            now += product_us
            cross_free = max(cross_free, now) + cross_us
            crossed.append(cross_free + 1.0)
            order.append((0, len(crossed) - 1))
            continue
        _, dims, _, size = units[first]
        now = max(now, ready[first]) + 0.04 * size
        level[first] += 1
        order.append((level[first], first))
        if level[first] in (1, 3):
            dim, piece = (dims[0], piece_us * size) if level[first] == 1 else (dims[1], piece_us * size / 4)
            ready[first] = max([send(dim, way, piece) for way in range(2)])
            rest[first] = max([send(dim, way, piece) for way in range(2)])
        elif level[first] in (2, 4):
            dim, piece = (dims[0], piece_us * size) if level[first] == 2 else (dims[1], piece_us * size / 4)
            ready[first] = max([rest[first]] + [send(dim, way, piece) for way in range(2)])
        elif level[first] == 5:
            piece = piece_us * size / 8
            ready[first] = max([send(dims[2], way, piece) for way in range(2)])
            ready[first] = max(ready[first], send(dims[2], first % 2, 2 * piece) + 0.7)
    return order


UNIT_LIST = make_units()
UNITS = len(UNIT_LIST)


def kernel(
    counts_ref,
    bucket_ref,
    hidden_ref,
    dout_ref,
    mean_ref,
    hidden_buf,
    lhs,
    dout_buf,
    acc,
    crossed,
    first_in,
    second_in,
    third_in,
    tally,
    tally_in,
    result,
    hidden_sem,
    dout_sem,
    cross_send,
    cross_recv,
    first_send,
    first_hop,
    first_rest,
    second_send,
    second_hop,
    second_rest,
    third_send,
    third_recv,
    tally_send,
    tally_recv,
    result_sem,
):
    me = tuple(lax.axis_index(axis) for axis in AXES)
    core = me[3]

    def shifted(dim, by):
        return lax.rem(me[dim] + by, 4)

    def peer(dim, by):
        return tuple(shifted(dim, by) if axis == dim else me[axis] for axis in range(4))

    partner = (me[0], me[1], me[2], 1 - core)

    barrier = pltpu.get_barrier_semaphore()
    pl.semaphore_signal(barrier, inc=1, device_id=partner, device_id_type=MESH)
    for dim in range(3):
        for by in (1, 2, 3):
            pl.semaphore_signal(barrier, inc=1, device_id=peer(dim, by), device_id_type=MESH)

    chunk = ROWS // HIDDEN_CHUNKS

    def hidden_copy(part):
        rows = pl.ds(part * chunk, chunk)
        return pltpu.make_async_copy(hidden_ref.at[rows], hidden_buf.at[rows], hidden_sem.at[part])

    def dout_copy(pair):
        slot = lax.rem(pair, DOUT_SLOTS)
        columns = pl.ds(pl.multiple_of(pair * PAIR, PAIR), PAIR)
        return pltpu.make_async_copy(dout_ref.at[:, columns], dout_buf.at[slot], dout_sem.at[slot])

    for part in range(HIDDEN_CHUNKS):
        hidden_copy(part).start()
    for pair in range(DOUT_SLOTS - 1):
        dout_copy(pair).start()

    own_count = counts_ref[0, bucket_ref[0]]

    for part in range(HIDDEN_CHUNKS):
        hidden_copy(part).wait()

        row = part * chunk
        position = lax.broadcasted_iota(jnp.int32, (chunk, 128), 0) + row
        live = jnp.where(position < own_count, 1.0, 0.0).astype(jnp.bfloat16)

        for unit in range(0, WIDTH, 128):
            masked = hidden_buf[pl.ds(row, chunk), pl.ds(unit, 128)] * live
            lhs[pl.ds(unit, 128), pl.ds(row, chunk)] = masked.T

    tally[0] = jnp.full((8, 128), own_count, jnp.int32).astype(jnp.float32)

    def remote(source, target, send, recv, device):
        return pltpu.make_async_remote_copy(
            src_ref=source,
            dst_ref=target,
            send_sem=send,
            recv_sem=recv,
            device_id=device,
            device_id_type=MESH,
        )

    def arrived(target, recv):
        remote(target, target, recv, recv, partner).wait_recv()

    def left(source, send):
        remote(source, source, send, send, partner).wait_send()

    def cross_copy(pair):
        slot = lax.rem(pair, THEIR_SLOTS)
        return remote(acc.at[slot], crossed.at[pair], cross_send.at[slot], cross_recv.at[pair], partner)

    def product(pair):
        slot = lax.rem(pair, DOUT_SLOTS)
        dout_copy(pair).wait()

        @pl.when(pair + (DOUT_SLOTS - 1) < PAIRS)
        def _():
            dout_copy(pair + (DOUT_SLOTS - 1)).start()

        theirs = lax.rem(pair, THEIR_SLOTS)
        mine = THEIR_SLOTS + pair
        place_0 = core * theirs + (1 - core) * mine
        place_1 = core * mine + (1 - core) * theirs
        for half in range(2):
            rows = pl.ds(half * (WIDTH // 2), WIDTH // 2)
            value = jnp.dot(lhs[rows, :], dout_buf[slot], preferred_element_type=jnp.float32)
            value = value.reshape(2, 4, 4, 2, 8, PAIR)
            acc[place_0, 2 * half : 2 * half + 2] = value[:, :, :, 0]
            acc[place_1, 2 * half : 2 * half + 2] = value[:, :, :, 1]

    def at(where):
        return tuple(where.get(dim, slice(None)) for dim in range(3))

    def half_of(side):
        return pl.ds(2 * side, 2)

    def first_region(order, place, side):
        cut = min(order[1], order[2])
        return at({order[0]: place, cut: half_of(side)})

    def second_region(order, place, side):
        return at({order[0]: me[order[0]], order[1]: place, order[2]: half_of(side)})

    def third_region(order, place):
        return at({order[0]: me[order[0]], order[1]: me[order[1]], order[2]: place})

    def gather(pair, size, region, terms):
        for step in range(size):
            spot = (THEIR_SLOTS + pair + step,) + region
            value = acc[spot]
            for ref, index in terms:
                value = value + ref[(pair + step,) + index]
            acc[spot] = value

    def first_copy(unit, kind):
        number, order, pair, size = unit
        by = (2, 2, 1, 3, 1, 3)[kind]
        side = (0, 1, 1, 0, 0, 1)[kind]
        region = first_region(order, shifted(order[0], by), side)
        recv = first_hop if kind < 2 else first_rest
        copy = remote(
            acc.at[(pl.ds(THEIR_SLOTS + pair, size),) + region],
            first_in.at[pl.ds(pair, size), kind],
            first_send,
            recv.at[number],
            peer(order[0], (1, 3)[kind % 2]),
        )
        return copy, region

    def second_copy(unit, kind):
        number, order, pair, size = unit
        by = (2, 2, 1, 3, 1, 3)[kind]
        side = (0, 1, 1, 0, 0, 1)[kind]
        region = second_region(order, shifted(order[1], by), side)
        recv = second_hop if kind < 2 else second_rest
        copy = remote(
            acc.at[(pl.ds(THEIR_SLOTS + pair, size),) + region],
            second_in.at[pl.ds(pair, size), kind],
            second_send,
            recv.at[number],
            peer(order[1], (1, 3)[kind % 2]),
        )
        return copy, region

    def third_copy(unit, by):
        number, order, pair, size = unit
        return remote(
            acc.at[(pl.ds(THEIR_SLOTS + pair, size),) + third_region(order, shifted(order[2], by))],
            third_in.at[pl.ds(pair, size), by - 1],
            third_send,
            third_recv.at[number],
            peer(order[2], by),
        )

    def stage_1(unit):
        number, order, pair, size = unit
        for step in range(size):
            arrived(crossed.at[pair + step], cross_recv.at[pair + step])
        for kind in range(4):
            copy, region = first_copy(unit, kind)
            gather(pair, size, region, ((crossed, region),))
            copy.start()

    def stage_2(unit):
        number, order, pair, size = unit
        arrived(first_in.at[pl.ds(pair, size), pl.ds(0, 2)], first_hop.at[number])
        for kind in (4, 5):
            copy, region = first_copy(unit, kind)
            gather(pair, size, region, ((crossed, region), (first_in, (kind - 4,))))
            copy.start()

    def stage_3(unit):
        number, order, pair, size = unit
        arrived(first_in.at[pl.ds(pair, size), pl.ds(2, 4)], first_rest.at[number])
        for side, (up, down) in enumerate(((4, 3), (2, 5))):
            region = first_region(order, me[order[0]], side)
            gather(pair, size, region, ((crossed, region), (first_in, (up,)), (first_in, (down,))))
        for kind in range(4):
            second_copy(unit, kind)[0].start()

    def stage_4(unit):
        number, order, pair, size = unit
        arrived(second_in.at[pl.ds(pair, size), pl.ds(0, 2)], second_hop.at[number])
        for kind in (4, 5):
            copy, region = second_copy(unit, kind)
            gather(pair, size, region, ((second_in, (kind - 4,)),))
            copy.start()

    def stage_5(unit):
        number, order, pair, size = unit
        arrived(second_in.at[pl.ds(pair, size), pl.ds(2, 4)], second_rest.at[number])
        for side, (up, down) in enumerate(((4, 3), (2, 5))):
            region = second_region(order, me[order[1]], side)
            gather(pair, size, region, ((second_in, (up,)), (second_in, (down,))))
        for by in (1, 2, 3):
            third_copy(unit, by).start()

    def result_copy(unit):
        number, order, pair, size = unit
        columns = pl.ds(pair * PAIR, size * PAIR)
        return pltpu.make_async_copy(result.at[:, columns], mean_ref.at[:, columns], result_sem)

    def stage_6(unit):
        number, order, pair, size = unit
        arrived(third_in.at[pl.ds(pair, size)], third_recv.at[number])
        region = third_region(order, me[order[2]])
        total = jnp.concatenate([tally[4]] * (PAIR // 128), axis=1)
        for step in range(size):
            value = acc[(THEIR_SLOTS + pair + step,) + region]
            for by in range(3):
                value = value + third_in[pair + step, by]
            result[:, pl.ds((pair + step) * PAIR, PAIR)] = value / total
        result_copy(unit).start()

    def tally_start(level):
        if level == 0:
            remote(tally.at[0], tally_in.at[0, 0], tally_send.at[0], tally_recv.at[0], partner).start()
        else:
            for by in (1, 2, 3):
                remote(
                    tally.at[level],
                    tally_in.at[level, by - 1],
                    tally_send.at[level],
                    tally_recv.at[level],
                    peer(level - 1, by),
                ).start()

    def tally_end(level):
        number = 1 if level == 0 else 3
        arrived(tally_in.at[level, pl.ds(0, number)], tally_recv.at[level])
        left(tally_in.at[level, pl.ds(0, number)], tally_send.at[level])
        value = tally[level]
        for by in range(number):
            value = value + tally_in[level, by]
        tally[level + 1] = value

    stages = (stage_1, stage_2, stage_3, stage_4, stage_5, stage_6)
    after = [[] for _ in range(PAIRS)]
    done = -1
    for level, number in list_schedule(UNIT_LIST):
        if level == 0:
            done = number
        else:
            after[done].append((level, number))

    product(0)
    pl.semaphore_wait(barrier, 10)
    cross_copy(0).start()
    tally_start(0)
    for block in range(0, PAIRS, BLOCK):

        def step(pair, carry, block=block):

            @pl.when(pair >= THEIR_SLOTS)
            def _():
                left(acc.at[lax.rem(pair, THEIR_SLOTS)], cross_send.at[lax.rem(pair, THEIR_SLOTS)])

            product(pair)
            cross_copy(pair).start()
            for offset in range(BLOCK):
                last = block + offset
                if last + 1 < PAIRS:

                    @pl.when(pair == last)
                    def _(last=last):
                        for level, number in after[last]:
                            stages[level - 1](UNIT_LIST[number])
                        if last in TALLY_AFTER:
                            tally_end(TALLY_AFTER.index(last))
                            if last < TALLY_AFTER[-1]:
                                tally_start(TALLY_AFTER.index(last) + 1)

            return carry

        lax.fori_loop(max(block, 1), block + BLOCK, step, 0)
    for level, number in after[PAIRS - 1]:
        stages[level - 1](UNIT_LIST[number])
    left(first_in, first_send)
    left(second_in, second_send)
    left(third_in, third_send)
    pltpu.make_async_copy(result, mean_ref, result_sem).wait()
    for slot in range(THEIR_SLOTS):
        left(acc.at[slot], cross_send.at[slot])


def reduced(counts, bucket_expert, hidden, dout):
    f32 = jnp.float32
    dma = pltpu.SemaphoreType.DMA
    smem = pl.BlockSpec(memory_space=pltpu.SMEM)
    away = pl.BlockSpec(memory_space=pl.ANY)
    return pl.pallas_call(
        kernel,
        out_shape=jax.ShapeDtypeStruct((8, PAIR * PAIRS), f32),
        in_specs=[smem, smem, away, away],
        out_specs=away,
        scratch_shapes=[
            pltpu.VMEM((ROWS, WIDTH), jnp.bfloat16),
            pltpu.VMEM((WIDTH, ROWS), jnp.bfloat16),
            pltpu.VMEM((DOUT_SLOTS, ROWS, PAIR), jnp.bfloat16),
            pltpu.VMEM((THEIR_SLOTS + PAIRS, 4, 4, 4, 8, PAIR), f32),
            pltpu.VMEM((PAIRS, 4, 4, 4, 8, PAIR), f32),
            pltpu.VMEM((PAIRS, 6, 2, 4, 8, PAIR), f32),
            pltpu.VMEM((PAIRS, 6, 2, 8, PAIR), f32),
            pltpu.VMEM((PAIRS, 3, 8, PAIR), f32),
            pltpu.VMEM((5, 8, 128), f32),
            pltpu.VMEM((4, 3, 8, 128), f32),
            pltpu.VMEM((8, PAIR * PAIRS), f32),
            dma((HIDDEN_CHUNKS,)),
            dma((DOUT_SLOTS,)),
            dma((THEIR_SLOTS,)),
            dma((PAIRS,)),
            dma,
            dma((UNITS,)),
            dma((UNITS,)),
            dma,
            dma((UNITS,)),
            dma((UNITS,)),
            dma,
            dma((UNITS,)),
            dma((4,)),
            dma((4,)),
            dma,
        ],
        compiler_params=pltpu.CompilerParams(
            collective_id=0, has_side_effects=True, vmem_limit_bytes=67043328
        ),
    )(counts, bucket_expert, hidden, dout)


def body(hidden, dout, counts, bucket_expert, param, momentum):
    grad = reduced(counts, bucket_expert, hidden, dout)
    blend = first_beta * momentum + (1.0 - first_beta) * grad
    direction = jnp.tanh(blend / soft_width) + decay_rate * param
    new_param = param - learn_rate * direction
    new_momentum = second_beta * momentum + (1.0 - second_beta) * grad
    return (new_param, new_momentum, direction)


def solution(mesh):
    split = Mesh(mesh.devices.reshape(4, 4, 4, 2), AXES)
    rows = P(AXES, None)
    return jax.shard_map(
        body,
        mesh=split,
        in_specs=(rows, rows, rows, P(), rows, rows),
        out_specs=(rows, rows, rows),
        check_vma=False,
    )
```

```python
import jax
import jax.numpy as jnp
from jax import lax
from jax.experimental import pallas as pl
from jax.experimental.pallas import tpu as pltpu
from jax.sharding import Mesh
from jax.sharding import PartitionSpec as P

AXES = ("x", "y", "z", "c")
MESH = pl.DeviceIdType.MESH

first_beta = 0.9
second_beta = 0.99
decay_rate = 0.1
learn_rate = 0.001
soft_width = 0.05

ROWS = 1536
WIDTH = 1024
PAIR = 256
PAIRS = 28
THEIR_SLOTS = 6
DOUT_SLOTS = 4
HIDDEN_CHUNKS = 6

X, Y, Z = range(3)
ORDERS = (
    (X, Y, Z), (Y, X, Z), (Z, Y, X), (X, Z, Y),
    (Y, Z, X), (Z, Y, X), (X, Y, Z), (Y, Z, X),
    (Z, Y, X), (X, Y, Z), (Y, Z, X), (X, Z, Y),
    (Z, Y, X), (X, Z, Y), (Z, X, Y), (Y, X, Z),
    (Y, X, Z), (Z, Y, X), (Z, Y, X), (X, Z, Y),
    (Y, X, Z), (X, Z, Y), (Y, X, Z), (X, Z, Y),
    (Z, Y, X), (X, Z, Y), (Y, X, Z), (Z, Y, X),
)
DIRECT = (22, 25, 26)
THIRD_ORDER = (
    2, 7, 10, 22, 9, 3, 15, 4, 12, 5, 11, 18, 19, 8,
    21, 26, 0, 16, 24, 14, 6, 1, 25, 27, 20, 13, 17, 23,
)
GROUP = 4
EVENTS = (
    (),
    (),
    (100,),
    (101,),
    (102,),
    (103,),
    (104,),
    (105, 200),
    (106, 201),
    (107, 202),
    (108, 203),
    (109, 204),
    (110, 205),
    (111,),
    (112, 206, 207, 302),
    (113, 208),
    (114,),
    (115, 209),
    (116, 210),
    (117, 212),
    (118, 211),
    (119, 402),
    (120,),
    (121, 214, 215),
    (122, 213),
    (123, 216, 217),
    (124,),
    (125, 126, 219, 127, 220, 218, 221, 315, 222, 224, 223, 316, 314, 226, 227, 307, 301, 310, 303, 304, 311,
        225, 309, 312, 305, 320, 318, 308, 319, 300, 322, 324, 502, 306, 321, 415, 313, 326, 327, 317, 409, 407,
        412, 410, 323, 416, 403, 405, 414, 404, 418, 401, 408, 411, 400, 419, 424, 421, 325, 420, 406, 413, 427,
        507, 510, 417, 423, 522, 509, 503, 515, 504, 512, 505, 511, 518, 519, 508, 521, 526, 500, 516, 524, 514,
        506, 501, 525, 527, 520, 513, 517, 523, 600, 601, 602, 603, 604, 605, 606),
)
BLOCK = 4
TALLY_AFTER = (3, 9, 15, 21)
UNITS = len(ORDERS)


def kernel(
    counts_ref,
    bucket_ref,
    hidden_ref,
    dout_ref,
    mean_ref,
    hidden_buf,
    lhs,
    dout_buf,
    acc,
    crossed,
    first_in,
    second_in,
    third_in,
    tally,
    tally_in,
    result,
    hidden_sem,
    dout_sem,
    cross_send,
    cross_recv,
    first_send,
    first_hop,
    first_rest,
    second_send,
    second_hop,
    second_rest,
    third_send,
    third_recv,
    tally_send,
    tally_recv,
    result_sem,
):
    me = tuple(lax.axis_index(axis) for axis in AXES)
    core = me[3]

    def shifted(dim, by):
        return lax.rem(me[dim] + by, 4)

    def peer(dim, by):
        return tuple(shifted(dim, by) if axis == dim else me[axis] for axis in range(4))

    partner = (me[0], me[1], me[2], 1 - core)

    barrier = pltpu.get_barrier_semaphore()
    pl.semaphore_signal(barrier, inc=1, device_id=partner, device_id_type=MESH)
    for dim in range(3):
        for by in (1, 2, 3):
            pl.semaphore_signal(barrier, inc=1, device_id=peer(dim, by), device_id_type=MESH)

    chunk = ROWS // HIDDEN_CHUNKS

    def hidden_copy(part):
        rows = pl.ds(part * chunk, chunk)
        return pltpu.make_async_copy(hidden_ref.at[rows], hidden_buf.at[rows], hidden_sem.at[part])

    def dout_copy(pair):
        slot = lax.rem(pair, DOUT_SLOTS)
        columns = pl.ds(pl.multiple_of(pair * PAIR, PAIR), PAIR)
        return pltpu.make_async_copy(dout_ref.at[:, columns], dout_buf.at[slot], dout_sem.at[slot])

    for part in range(HIDDEN_CHUNKS):
        hidden_copy(part).start()
    for pair in range(DOUT_SLOTS - 1):
        dout_copy(pair).start()

    own_count = counts_ref[0, bucket_ref[0]]

    for part in range(HIDDEN_CHUNKS):
        hidden_copy(part).wait()

        row = part * chunk
        position = lax.broadcasted_iota(jnp.int32, (chunk, 128), 0) + row
        live = jnp.where(position < own_count, 1.0, 0.0).astype(jnp.bfloat16)

        for unit in range(0, WIDTH, 128):
            masked = hidden_buf[pl.ds(row, chunk), pl.ds(unit, 128)] * live
            lhs[pl.ds(unit, 128), pl.ds(row, chunk)] = masked.T

    tally[0] = jnp.full((8, 128), own_count, jnp.int32).astype(jnp.float32)

    def remote(source, target, send, recv, device):
        return pltpu.make_async_remote_copy(
            src_ref=source,
            dst_ref=target,
            send_sem=send,
            recv_sem=recv,
            device_id=device,
            device_id_type=MESH,
        )

    def arrived(target, recv):
        remote(target, target, recv, recv, partner).wait_recv()

    def left(source, send):
        remote(source, source, send, send, partner).wait_send()

    def cross_copy(pair):
        slot = lax.rem(pair, THEIR_SLOTS)
        return remote(acc.at[slot], crossed.at[pair], cross_send.at[slot], cross_recv.at[pair], partner)

    def product(pair):
        slot = lax.rem(pair, DOUT_SLOTS)
        dout_copy(pair).wait()

        @pl.when(pair + (DOUT_SLOTS - 1) < PAIRS)
        def _():
            dout_copy(pair + (DOUT_SLOTS - 1)).start()

        theirs = lax.rem(pair, THEIR_SLOTS)
        mine = THEIR_SLOTS + pair
        place_0 = core * theirs + (1 - core) * mine
        place_1 = core * mine + (1 - core) * theirs
        for half in range(2):
            rows = pl.ds(half * (WIDTH // 2), WIDTH // 2)
            value = jnp.dot(lhs[rows, :], dout_buf[slot], preferred_element_type=jnp.float32)
            value = value.reshape(2, 4, 4, 2, 8, PAIR)
            acc[place_0, 2 * half : 2 * half + 2] = value[:, :, :, 0]
            acc[place_1, 2 * half : 2 * half + 2] = value[:, :, :, 1]

    def at(where):
        return tuple(where.get(dim, slice(None)) for dim in range(3))

    def half_of(side):
        return pl.ds(2 * side, 2)

    def first_region(order, place, side):
        cut = min(order[1], order[2])
        return at({order[0]: place, cut: half_of(side)})

    def second_region(order, place, side):
        return at({order[0]: me[order[0]], order[1]: place, order[2]: half_of(side)})

    def third_region(order, place):
        return at({order[0]: me[order[0]], order[1]: me[order[1]], order[2]: place})

    def gather(pair, size, region, terms):
        for step in range(size):
            spot = (THEIR_SLOTS + pair + step,) + region
            value = acc[spot]
            for ref, index in terms:
                value = value + ref[(pair + step,) + index]
            acc[spot] = value

    def first_copy(unit, kind):
        number, order, pair, size = unit
        by = (2, 2, 1, 3, 1, 3)[kind]
        side = (0, 1, 1, 0, 0, 1)[kind]
        region = first_region(order, shifted(order[0], by), side)
        recv = first_hop if kind < 2 else first_rest
        copy = remote(
            acc.at[(pl.ds(THEIR_SLOTS + pair, size),) + region],
            first_in.at[pl.ds(pair, size), kind],
            first_send,
            recv.at[number],
            peer(order[0], (1, 3)[kind % 2]),
        )
        return copy, region

    def second_copy(unit, kind):
        number, order, pair, size = unit
        by = (2, 2, 1, 3, 1, 3)[kind]
        side = (0, 1, 1, 0, 0, 1)[kind]
        region = second_region(order, shifted(order[1], by), side)
        recv = second_hop if kind < 2 else second_rest
        copy = remote(
            acc.at[(pl.ds(THEIR_SLOTS + pair, size),) + region],
            second_in.at[pl.ds(pair, size), kind],
            second_send,
            recv.at[number],
            peer(order[1], (1, 3)[kind % 2]),
        )
        return copy, region

    def direct_copy(unit, by, side):
        number, order, pair, size = unit
        region = second_region(order, shifted(order[1], by), side)
        return remote(
            acc.at[(pl.ds(THEIR_SLOTS + pair, size),) + region],
            second_in.at[pl.ds(pair, size), 2 * (by - 1) + side],
            second_send,
            second_rest.at[number],
            peer(order[1], by),
        )

    def third_copy(unit, by):
        number, order, pair, size = unit
        return remote(
            acc.at[(pl.ds(THEIR_SLOTS + pair, size),) + third_region(order, shifted(order[2], by))],
            third_in.at[pl.ds(THIRD_ORDER.index(number), size), by - 1],
            third_send,
            third_recv.at[THIRD_ORDER.index(number) // GROUP],
            peer(order[2], by),
        )

    def stage_1(unit):
        number, order, pair, size = unit
        for step in range(size):
            arrived(crossed.at[pair + step], cross_recv.at[pair + step])
        for kind in range(4):
            copy, region = first_copy(unit, kind)
            gather(pair, size, region, ((crossed, region),))
            copy.start()

    def stage_2(unit):
        number, order, pair, size = unit
        arrived(first_in.at[pl.ds(pair, size), pl.ds(0, 2)], first_hop.at[number])
        for kind in (4, 5):
            copy, region = first_copy(unit, kind)
            gather(pair, size, region, ((crossed, region), (first_in, (kind - 4,))))
            copy.start()

    def stage_3(unit):
        number, order, pair, size = unit
        arrived(first_in.at[pl.ds(pair, size), pl.ds(2, 4)], first_rest.at[number])
        for side, (up, down) in enumerate(((4, 3), (2, 5))):
            region = first_region(order, me[order[0]], side)
            gather(pair, size, region, ((crossed, region), (first_in, (up,)), (first_in, (down,))))
        if number in DIRECT:
            for by in (1, 2, 3):
                for side in range(2):
                    direct_copy(unit, by, side).start()
        else:
            for kind in range(4):
                second_copy(unit, kind)[0].start()

    def stage_4(unit):
        number, order, pair, size = unit
        arrived(second_in.at[pl.ds(pair, size), pl.ds(0, 2)], second_hop.at[number])
        for kind in (4, 5):
            copy, region = second_copy(unit, kind)
            gather(pair, size, region, ((second_in, (kind - 4,)),))
            copy.start()

    def stage_5(unit):
        number, order, pair, size = unit
        if number in DIRECT:
            arrived(second_in.at[pl.ds(pair, size)], second_rest.at[number])
        else:
            arrived(second_in.at[pl.ds(pair, size), pl.ds(2, 4)], second_rest.at[number])
        for side, (up, down) in enumerate(((4, 3), (2, 5))):
            region = second_region(order, me[order[1]], side)
            if number in DIRECT:
                gather(pair, size, region, tuple((second_in, (2 * by + side,)) for by in range(3)))
            else:
                gather(pair, size, region, ((second_in, (up,)), (second_in, (down,))))
        for by in (1, 2, 3):
            third_copy(unit, by).start()

    def result_copy(unit):
        number, order, pair, size = unit
        columns = pl.ds(pair * PAIR, size * PAIR)
        return pltpu.make_async_copy(result.at[:, columns], mean_ref.at[:, columns], result_sem)

    def stage_6(group):
        arrived(third_in.at[pl.ds(group * GROUP, GROUP)], third_recv.at[group])
        total = jnp.concatenate([tally[4]] * (PAIR // 128), axis=1)
        for rank in range(group * GROUP, (group + 1) * GROUP):
            unit = unit_of(THIRD_ORDER[rank])
            number, order, pair, size = unit
            value = acc[(THEIR_SLOTS + pair,) + third_region(order, me[order[2]])]
            for by in range(3):
                value = value + third_in[rank, by]
            result[:, pl.ds(pair * PAIR, PAIR)] = value / total
            result_copy(unit).start()

    def tally_start(level):
        if level == 0:
            remote(tally.at[0], tally_in.at[0, 0], tally_send.at[0], tally_recv.at[0], partner).start()
        else:
            for by in (1, 2, 3):
                remote(
                    tally.at[level],
                    tally_in.at[level, by - 1],
                    tally_send.at[level],
                    tally_recv.at[level],
                    peer(level - 1, by),
                ).start()

    def tally_end(level):
        number = 1 if level == 0 else 3
        arrived(tally_in.at[level, pl.ds(0, number)], tally_recv.at[level])
        left(tally_in.at[level, pl.ds(0, number)], tally_send.at[level])
        value = tally[level]
        for by in range(number):
            value = value + tally_in[level, by]
        tally[level + 1] = value

    def unit_of(number):
        return number, ORDERS[number], number, 1

    stages = (stage_1, stage_2, stage_3, stage_4, stage_5)

    def events(last):
        for event in EVENTS[last]:
            level, number = divmod(event, 100)
            if level == 6:
                stage_6(number)
            else:
                stages[level - 1](unit_of(number))

    product(0)
    pl.semaphore_wait(barrier, 10)
    cross_copy(0).start()
    tally_start(0)
    for block in range(0, PAIRS, BLOCK):

        def step(pair, carry, block=block):

            @pl.when(pair >= THEIR_SLOTS)
            def _():
                left(acc.at[lax.rem(pair, THEIR_SLOTS)], cross_send.at[lax.rem(pair, THEIR_SLOTS)])

            product(pair)
            cross_copy(pair).start()
            for offset in range(BLOCK):
                last = block + offset
                if last + 1 < PAIRS:

                    @pl.when(pair == last)
                    def _(last=last):
                        events(last)
                        if last in TALLY_AFTER:
                            tally_end(TALLY_AFTER.index(last))
                            if last < TALLY_AFTER[-1]:
                                tally_start(TALLY_AFTER.index(last) + 1)

            return carry

        lax.fori_loop(max(block, 1), block + BLOCK, step, 0)
    events(PAIRS - 1)
    left(first_in, first_send)
    left(second_in, second_send)
    left(third_in, third_send)
    pltpu.make_async_copy(result, mean_ref, result_sem).wait()
    for slot in range(THEIR_SLOTS):
        left(acc.at[slot], cross_send.at[slot])


def reduced(counts, bucket_expert, hidden, dout):
    f32 = jnp.float32
    dma = pltpu.SemaphoreType.DMA
    smem = pl.BlockSpec(memory_space=pltpu.SMEM)
    away = pl.BlockSpec(memory_space=pl.ANY)
    return pl.pallas_call(
        kernel,
        out_shape=jax.ShapeDtypeStruct((8, PAIR * PAIRS), f32),
        in_specs=[smem, smem, away, away],
        out_specs=away,
        scratch_shapes=[
            pltpu.VMEM((ROWS, WIDTH), jnp.bfloat16),
            pltpu.VMEM((WIDTH, ROWS), jnp.bfloat16),
            pltpu.VMEM((DOUT_SLOTS, ROWS, PAIR), jnp.bfloat16),
            pltpu.VMEM((THEIR_SLOTS + PAIRS, 4, 4, 4, 8, PAIR), f32),
            pltpu.VMEM((PAIRS, 4, 4, 4, 8, PAIR), f32),
            pltpu.VMEM((PAIRS, 6, 2, 4, 8, PAIR), f32),
            pltpu.VMEM((PAIRS, 6, 2, 8, PAIR), f32),
            pltpu.VMEM((PAIRS, 3, 8, PAIR), f32),
            pltpu.VMEM((5, 8, 128), f32),
            pltpu.VMEM((4, 3, 8, 128), f32),
            pltpu.VMEM((8, PAIR * PAIRS), f32),
            dma((HIDDEN_CHUNKS,)),
            dma((DOUT_SLOTS,)),
            dma((THEIR_SLOTS,)),
            dma((PAIRS,)),
            dma,
            dma((UNITS,)),
            dma((UNITS,)),
            dma,
            dma((UNITS,)),
            dma((UNITS,)),
            dma,
            dma((UNITS // GROUP,)),
            dma((4,)),
            dma((4,)),
            dma,
        ],
        compiler_params=pltpu.CompilerParams(
            collective_id=0, has_side_effects=True, vmem_limit_bytes=67043328
        ),
    )(counts, bucket_expert, hidden, dout)


def body(hidden, dout, counts, bucket_expert, param, momentum):
    grad = reduced(counts, bucket_expert, hidden, dout)
    blend = first_beta * momentum + (1.0 - first_beta) * grad
    direction = jnp.tanh(blend / soft_width) + decay_rate * param
    new_param = param - learn_rate * direction
    new_momentum = second_beta * momentum + (1.0 - second_beta) * grad
    return (new_param, new_momentum, direction)


def solution(mesh):
    split = Mesh(mesh.devices.reshape(4, 4, 4, 2), AXES)
    rows = P(AXES, None)
    return jax.shard_map(
        body,
        mesh=split,
        in_specs=(rows, rows, rows, P(), rows, rows),
        out_specs=(rows, rows, rows),
        check_vma=False,
    )
```

```python
import jax
import jax.numpy as jnp
from jax import lax
from jax.experimental import pallas as pl
from jax.experimental.pallas import tpu as pltpu
from jax.sharding import Mesh
from jax.sharding import PartitionSpec as P

AXES = ("x", "y", "z", "c")
MESH = pl.DeviceIdType.MESH

first_beta = 0.9
second_beta = 0.99
decay_rate = 0.1
learn_rate = 0.001
soft_width = 0.05

ROWS = 1536
WIDTH = 1024
PAIR = 256
PAIRS = 28
THEIR_SLOTS = 6
DOUT_SLOTS = 4
HIDDEN_CHUNKS = 6

X, Y, Z = range(3)
ORDERS = (
    (X, Y, Z), (Y, X, Z), (Z, X, Y), (X, Z, Y),
    (Y, X, Z), (Z, X, Y), (X, Z, Y), (Y, X, Z),
    (Z, Y, X), (X, Y, Z), (X, Y, Z), (Y, X, Z),
    (Z, Y, X), (Y, Z, X), (Z, Y, X), (Y, Z, X),
    (Y, X, Z), (X, Z, Y), (Y, X, Z), (Z, Y, X),
    (X, Z, Y), (Y, Z, X), (X, Z, Y), (Z, Y, X),
    (X, Z, Y), (Z, Y, X), (Z, Y, X), (X, Y, Z),
)
DIRECT = (7, 24, 27)
THIRD_ORDER = (
    9, 13, 4, 17, 0, 19, 12, 1, 14, 24, 8, 15, 3, 7,
    20, 27, 6, 16, 23, 22, 2, 25, 21, 18, 10, 5, 26, 11,
)
GROUP = 4
EVENTS = (
    (),
    (),
    (100,),
    (101,),
    (102,),
    (103,),
    (104,),
    (105, 200),
    (106, 201),
    (107, 202),
    (108, 203),
    (109, 204),
    (110, 205, 300),
    (111,),
    (112, 206),
    (113, 207),
    (114, 208),
    (115, 209, 304, 400),
    (116,),
    (117, 211, 212),
    (118, 210),
    (119,),
    (120, 213, 214),
    (121,),
    (122, 309, 404),
    (123, 215),
    (124, 217),
    (125, 219, 126, 216, 127, 220, 223, 222, 218, 225, 313, 224, 301, 221, 319, 312, 226, 314, 317, 409, 227,
        315, 308, 303, 323, 316, 302, 325, 320, 413, 318, 306, 322, 305, 310, 321, 326, 311, 419, 417, 324, 412,
        415, 401, 414, 403, 307, 509, 420, 408, 327, 513, 416, 423, 406, 402, 425, 422, 418, 410, 421, 504, 405,
        426, 517, 500, 411, 519, 512, 501, 514, 524, 508, 515, 503, 507, 520, 527, 506, 516, 523, 522, 502, 525,
        521, 518, 510, 505, 526, 511, 600, 601, 602, 603, 604, 605, 606),
)
BLOCK = 4
TALLY_AFTER = (3, 9, 15, 21)
UNITS = len(ORDERS)


def kernel(
    counts_hbm,
    bucket_hbm,
    hidden_ref,
    dout_ref,
    mean_ref,
    hidden_buf,
    lhs,
    dout_buf,
    acc,
    crossed,
    first_in,
    second_in,
    third_in,
    tally,
    tally_in,
    result,
    counts_ref,
    bucket_ref,
    scalar_sem,
    hidden_sem,
    dout_sem,
    cross_send,
    cross_recv,
    first_send,
    first_hop,
    first_rest,
    second_send,
    second_hop,
    second_rest,
    third_send,
    third_recv,
    tally_send,
    tally_recv,
    result_sem,
):
    me = tuple(lax.axis_index(axis) for axis in AXES)
    core = me[3]

    def shifted(dim, by):
        return lax.rem(me[dim] + by, 4)

    def peer(dim, by):
        return tuple(shifted(dim, by) if axis == dim else me[axis] for axis in range(4))

    partner = (me[0], me[1], me[2], 1 - core)

    chunk = ROWS // HIDDEN_CHUNKS

    def hidden_copy(part):
        rows = pl.ds(part * chunk, chunk)
        return pltpu.make_async_copy(hidden_ref.at[rows], hidden_buf.at[rows], hidden_sem.at[part])

    def dout_copy(pair):
        slot = lax.rem(pair, DOUT_SLOTS)
        columns = pl.ds(pl.multiple_of(pair * PAIR, PAIR), PAIR)
        return pltpu.make_async_copy(dout_ref.at[:, columns], dout_buf.at[slot], dout_sem.at[slot])

    scalars = (
        pltpu.make_async_copy(counts_hbm, counts_ref, scalar_sem.at[0]),
        pltpu.make_async_copy(bucket_hbm, bucket_ref, scalar_sem.at[1]),
    )
    for copy in scalars:
        copy.start()
    hidden_copy(0).start()

    barrier = pltpu.get_barrier_semaphore()
    pl.semaphore_signal(barrier, inc=1, device_id=partner, device_id_type=MESH)
    for dim in range(3):
        for by in (1, 2, 3):
            pl.semaphore_signal(barrier, inc=1, device_id=peer(dim, by), device_id_type=MESH)

    for part in range(1, HIDDEN_CHUNKS):
        hidden_copy(part).start()
    for pair in range(DOUT_SLOTS - 1):
        dout_copy(pair).start()

    for copy in scalars:
        copy.wait()
    own_count = counts_ref[0, bucket_ref[0]]

    for part in range(HIDDEN_CHUNKS):
        hidden_copy(part).wait()

        row = part * chunk
        position = lax.broadcasted_iota(jnp.int32, (chunk, 128), 0) + row
        live = jnp.where(position < own_count, 1.0, 0.0).astype(jnp.bfloat16)

        for unit in range(0, WIDTH, 128):
            masked = hidden_buf[pl.ds(row, chunk), pl.ds(unit, 128)] * live
            lhs[pl.ds(unit, 128), pl.ds(row, chunk)] = masked.T

    tally[0] = jnp.full((8, 128), own_count, jnp.int32).astype(jnp.float32)

    def remote(source, target, send, recv, device):
        return pltpu.make_async_remote_copy(
            src_ref=source,
            dst_ref=target,
            send_sem=send,
            recv_sem=recv,
            device_id=device,
            device_id_type=MESH,
        )

    def arrived(target, recv):
        remote(target, target, recv, recv, partner).wait_recv()

    def left(source, send):
        remote(source, source, send, send, partner).wait_send()

    def cross_copy(pair):
        slot = lax.rem(pair, THEIR_SLOTS)
        return remote(acc.at[slot], crossed.at[pair], cross_send.at[slot], cross_recv.at[pair], partner)

    def product(pair):
        slot = lax.rem(pair, DOUT_SLOTS)
        dout_copy(pair).wait()

        @pl.when(pair + (DOUT_SLOTS - 1) < PAIRS)
        def _():
            dout_copy(pair + (DOUT_SLOTS - 1)).start()

        theirs = lax.rem(pair, THEIR_SLOTS)
        mine = THEIR_SLOTS + pair
        place_0 = core * theirs + (1 - core) * mine
        place_1 = core * mine + (1 - core) * theirs
        for half in range(2):
            rows = pl.ds(half * (WIDTH // 2), WIDTH // 2)
            value = jnp.dot(lhs[rows, :], dout_buf[slot], preferred_element_type=jnp.float32)
            value = value.reshape(2, 4, 4, 2, 8, PAIR)
            acc[place_0, 2 * half : 2 * half + 2] = value[:, :, :, 0]
            acc[place_1, 2 * half : 2 * half + 2] = value[:, :, :, 1]

    def at(where):
        return tuple(where.get(dim, slice(None)) for dim in range(3))

    def half_of(side):
        return pl.ds(2 * side, 2)

    def first_region(order, place, side):
        cut = min(order[1], order[2])
        return at({order[0]: place, cut: half_of(side)})

    def second_region(order, place, side):
        return at({order[0]: me[order[0]], order[1]: place, order[2]: half_of(side)})

    def third_region(order, place):
        return at({order[0]: me[order[0]], order[1]: me[order[1]], order[2]: place})

    def gather(pair, size, region, terms):
        for step in range(size):
            spot = (THEIR_SLOTS + pair + step,) + region
            value = acc[spot]
            for ref, index in terms:
                value = value + ref[(pair + step,) + index]
            acc[spot] = value

    def first_copy(unit, kind):
        number, order, pair, size = unit
        by = (2, 2, 1, 3, 1, 3)[kind]
        side = (0, 1, 1, 0, 0, 1)[kind]
        region = first_region(order, shifted(order[0], by), side)
        recv = first_hop if kind < 2 else first_rest
        copy = remote(
            acc.at[(pl.ds(THEIR_SLOTS + pair, size),) + region],
            first_in.at[pl.ds(pair, size), kind],
            first_send,
            recv.at[number],
            peer(order[0], (1, 3)[kind % 2]),
        )
        return copy, region

    def second_copy(unit, kind):
        number, order, pair, size = unit
        by = (2, 2, 1, 3, 1, 3)[kind]
        side = (0, 1, 1, 0, 0, 1)[kind]
        region = second_region(order, shifted(order[1], by), side)
        recv = second_hop if kind < 2 else second_rest
        copy = remote(
            acc.at[(pl.ds(THEIR_SLOTS + pair, size),) + region],
            second_in.at[pl.ds(pair, size), kind],
            second_send,
            recv.at[number],
            peer(order[1], (1, 3)[kind % 2]),
        )
        return copy, region

    def direct_copy(unit, by, side):
        number, order, pair, size = unit
        region = second_region(order, shifted(order[1], by), side)
        return remote(
            acc.at[(pl.ds(THEIR_SLOTS + pair, size),) + region],
            second_in.at[pl.ds(pair, size), 2 * (by - 1) + side],
            second_send,
            second_rest.at[number],
            peer(order[1], by),
        )

    def third_copy(unit, by):
        number, order, pair, size = unit
        return remote(
            acc.at[(pl.ds(THEIR_SLOTS + pair, size),) + third_region(order, shifted(order[2], by))],
            third_in.at[pl.ds(THIRD_ORDER.index(number), size), by - 1],
            third_send,
            third_recv.at[THIRD_ORDER.index(number) // GROUP],
            peer(order[2], by),
        )

    def stage_1(unit):
        number, order, pair, size = unit
        for step in range(size):
            arrived(crossed.at[pair + step], cross_recv.at[pair + step])
        for kind in range(4):
            copy, region = first_copy(unit, kind)
            gather(pair, size, region, ((crossed, region),))
            copy.start()

    def stage_2(unit):
        number, order, pair, size = unit
        arrived(first_in.at[pl.ds(pair, size), pl.ds(0, 2)], first_hop.at[number])
        for kind in (4, 5):
            copy, region = first_copy(unit, kind)
            gather(pair, size, region, ((crossed, region), (first_in, (kind - 4,))))
            copy.start()

    def stage_3(unit):
        number, order, pair, size = unit
        arrived(first_in.at[pl.ds(pair, size), pl.ds(2, 4)], first_rest.at[number])
        for side, (up, down) in enumerate(((4, 3), (2, 5))):
            region = first_region(order, me[order[0]], side)
            gather(pair, size, region, ((crossed, region), (first_in, (up,)), (first_in, (down,))))
        if number in DIRECT:
            for by in (1, 2, 3):
                for side in range(2):
                    direct_copy(unit, by, side).start()
        else:
            for kind in range(4):
                second_copy(unit, kind)[0].start()

    def stage_4(unit):
        number, order, pair, size = unit
        arrived(second_in.at[pl.ds(pair, size), pl.ds(0, 2)], second_hop.at[number])
        for kind in (4, 5):
            copy, region = second_copy(unit, kind)
            gather(pair, size, region, ((second_in, (kind - 4,)),))
            copy.start()

    def stage_5(unit):
        number, order, pair, size = unit
        if number in DIRECT:
            arrived(second_in.at[pl.ds(pair, size)], second_rest.at[number])
        else:
            arrived(second_in.at[pl.ds(pair, size), pl.ds(2, 4)], second_rest.at[number])
        for side, (up, down) in enumerate(((4, 3), (2, 5))):
            region = second_region(order, me[order[1]], side)
            if number in DIRECT:
                gather(pair, size, region, tuple((second_in, (2 * by + side,)) for by in range(3)))
            else:
                gather(pair, size, region, ((second_in, (up,)), (second_in, (down,))))
        for by in (1, 2, 3):
            third_copy(unit, by).start()

    def result_copy(unit):
        number, order, pair, size = unit
        columns = pl.ds(pair * PAIR, size * PAIR)
        return pltpu.make_async_copy(result.at[:, columns], mean_ref.at[:, columns], result_sem)

    def stage_6(group):
        arrived(third_in.at[pl.ds(group * GROUP, GROUP)], third_recv.at[group])
        total = jnp.concatenate([tally[4]] * (PAIR // 128), axis=1)
        for rank in range(group * GROUP, (group + 1) * GROUP):
            unit = unit_of(THIRD_ORDER[rank])
            number, order, pair, size = unit
            value = acc[(THEIR_SLOTS + pair,) + third_region(order, me[order[2]])]
            for by in range(3):
                value = value + third_in[rank, by]
            result[:, pl.ds(pair * PAIR, PAIR)] = value / total
            result_copy(unit).start()

    def tally_start(level):
        if level == 0:
            remote(tally.at[0], tally_in.at[0, 0], tally_send.at[0], tally_recv.at[0], partner).start()
        else:
            for by in (1, 2, 3):
                remote(
                    tally.at[level],
                    tally_in.at[level, by - 1],
                    tally_send.at[level],
                    tally_recv.at[level],
                    peer(level - 1, by),
                ).start()

    def tally_end(level):
        number = 1 if level == 0 else 3
        arrived(tally_in.at[level, pl.ds(0, number)], tally_recv.at[level])
        left(tally_in.at[level, pl.ds(0, number)], tally_send.at[level])
        value = tally[level]
        for by in range(number):
            value = value + tally_in[level, by]
        tally[level + 1] = value

    def unit_of(number):
        return number, ORDERS[number], number, 1

    stages = (stage_1, stage_2, stage_3, stage_4, stage_5)

    def events(last):
        for event in EVENTS[last]:
            level, number = divmod(event, 100)
            if level == 6:
                stage_6(number)
            else:
                stages[level - 1](unit_of(number))

    product(0)
    pl.semaphore_wait(barrier, 10)
    cross_copy(0).start()
    tally_start(0)
    for block in range(0, PAIRS, BLOCK):

        def step(pair, carry, block=block):

            @pl.when(pair >= THEIR_SLOTS)
            def _():
                left(acc.at[lax.rem(pair, THEIR_SLOTS)], cross_send.at[lax.rem(pair, THEIR_SLOTS)])

            product(pair)
            cross_copy(pair).start()
            for offset in range(BLOCK):
                last = block + offset
                if last + 1 < PAIRS:

                    @pl.when(pair == last)
                    def _(last=last):
                        events(last)
                        if last in TALLY_AFTER:
                            tally_end(TALLY_AFTER.index(last))
                            if last < TALLY_AFTER[-1]:
                                tally_start(TALLY_AFTER.index(last) + 1)

            return carry

        lax.fori_loop(max(block, 1), block + BLOCK, step, 0)
    events(PAIRS - 1)
    left(first_in, first_send)
    left(second_in, second_send)
    left(third_in, third_send)
    pltpu.make_async_copy(result, mean_ref, result_sem).wait()
    for slot in range(THEIR_SLOTS):
        left(acc.at[slot], cross_send.at[slot])


def reduced(counts, bucket_expert, hidden, dout):
    f32 = jnp.float32
    dma = pltpu.SemaphoreType.DMA
    away = pl.BlockSpec(memory_space=pl.ANY)
    return pl.pallas_call(
        kernel,
        out_shape=jax.ShapeDtypeStruct((8, PAIR * PAIRS), f32),
        in_specs=[away] * 4,
        out_specs=away,
        scratch_shapes=[
            pltpu.VMEM((ROWS, WIDTH), jnp.bfloat16),
            pltpu.VMEM((WIDTH, ROWS), jnp.bfloat16),
            pltpu.VMEM((DOUT_SLOTS, ROWS, PAIR), jnp.bfloat16),
            pltpu.VMEM((THEIR_SLOTS + PAIRS, 4, 4, 4, 8, PAIR), f32),
            pltpu.VMEM((PAIRS, 4, 4, 4, 8, PAIR), f32),
            pltpu.VMEM((PAIRS, 6, 2, 4, 8, PAIR), f32),
            pltpu.VMEM((PAIRS, 6, 2, 8, PAIR), f32),
            pltpu.VMEM((PAIRS, 3, 8, PAIR), f32),
            pltpu.VMEM((5, 8, 128), f32),
            pltpu.VMEM((4, 3, 8, 128), f32),
            pltpu.VMEM((8, PAIR * PAIRS), f32),
            pltpu.SMEM((1, 256), jnp.int32),
            pltpu.SMEM((1,), jnp.int32),
            dma((2,)),
            dma((HIDDEN_CHUNKS,)),
            dma((DOUT_SLOTS,)),
            dma((THEIR_SLOTS,)),
            dma((PAIRS,)),
            dma,
            dma((UNITS,)),
            dma((UNITS,)),
            dma,
            dma((UNITS,)),
            dma((UNITS,)),
            dma,
            dma((UNITS // GROUP,)),
            dma((4,)),
            dma((4,)),
            dma,
        ],
        compiler_params=pltpu.CompilerParams(
            collective_id=0, has_side_effects=True, vmem_limit_bytes=67043328
        ),
    )(counts, bucket_expert, hidden, dout)


def body(hidden, dout, counts, bucket_expert, param, momentum):
    grad = reduced(counts, bucket_expert, hidden, dout)
    blend = first_beta * momentum + (1.0 - first_beta) * grad
    direction = jnp.tanh(blend / soft_width) + decay_rate * param
    new_param = param - learn_rate * direction
    new_momentum = second_beta * momentum + (1.0 - second_beta) * grad
    return (new_param, new_momentum, direction)


def solution(mesh):
    split = Mesh(mesh.devices.reshape(4, 4, 4, 2), AXES)
    rows = P(AXES, None)
    return jax.shard_map(
        body,
        mesh=split,
        in_specs=(rows, rows, rows, P(), rows, rows),
        out_specs=(rows, rows, rows),
        check_vma=False,
    )
```

```python
import jax
import jax.numpy as jnp
from jax import lax
from jax.experimental import pallas as pl
from jax.experimental.pallas import tpu as pltpu
from jax.sharding import Mesh
from jax.sharding import PartitionSpec as P

AXES = ("x", "y", "z", "c")
MESH = pl.DeviceIdType.MESH

first_beta = 0.9
second_beta = 0.99
decay_rate = 0.1
learn_rate = 0.001
soft_width = 0.05

ROWS = 1536
WIDTH = 1024
PAIR = 256
PAIRS = 28
THEIR_SLOTS = 6
DOUT_SLOTS = 4
HIDDEN_CHUNKS = 6

X, Y, Z = range(3)
ORDERS = (
    (X, Y, Z), (Y, X, Z), (Z, X, Y), (X, Z, Y),
    (Y, X, Z), (Z, X, Y), (X, Z, Y), (Y, X, Z),
    (Z, Y, X), (X, Y, Z), (X, Y, Z), (Y, X, Z),
    (Z, Y, X), (Y, Z, X), (Z, Y, X), (Y, Z, X),
    (Y, X, Z), (X, Z, Y), (Y, X, Z), (Z, Y, X),
    (X, Z, Y), (Y, Z, X), (X, Z, Y), (Z, Y, X),
    (X, Z, Y), (Z, Y, X), (Z, Y, X), (X, Y, Z),
)
DIRECT = (7, 24, 27)
THIRD_ORDER = (
    9, 13, 4, 17, 0, 19, 12, 1, 14, 24, 8, 15, 3, 7,
    20, 27, 6, 16, 23, 22, 2, 25, 21, 18, 10, 5, 26, 11,
)
GROUP = 4
EVENTS = (
    (),
    (),
    (100,),
    (101,),
    (102,),
    (103,),
    (104,),
    (105, 200),
    (106, 201),
    (107, 202),
    (108, 203),
    (109, 204),
    (110, 205, 300),
    (111,),
    (112, 206),
    (113, 207),
    (114, 208),
    (115, 209, 304, 400),
    (116,),
    (117, 211, 212),
    (118, 210),
    (119,),
    (120, 213, 214),
    (121,),
    (122, 309, 404),
    (123, 215),
    (124, 217),
    (125, 219, 126, 216, 127, 220, 223, 222, 218, 225, 313, 224, 301, 221, 319, 312, 226, 314, 317, 409, 227,
        315, 308, 303, 323, 316, 302, 325, 320, 413, 318, 306, 322, 305, 310, 321, 326, 311, 419, 417, 324, 412,
        415, 401, 414, 403, 307, 509, 420, 408, 327, 513, 416, 423, 406, 402, 425, 422, 418, 410, 421, 504, 405,
        426, 517, 500, 411, 519, 512, 501, 514, 524, 508, 515, 503, 507, 520, 527, 506, 516, 523, 522, 502, 525,
        521, 518, 510, 505, 526, 511, 600, 601, 602, 603, 604, 605, 606),
)
BLOCK = 4
TALLY_AFTER = (3, 9, 15, 21)
UNITS = len(ORDERS)


def kernel(
    counts_hbm,
    bucket_hbm,
    hidden_ref,
    dout_ref,
    mean_ref,
    hidden_buf,
    lhs,
    dout_buf,
    acc,
    crossed,
    first_in,
    second_in,
    third_in,
    tally,
    tally_in,
    result,
    counts_ref,
    bucket_ref,
    scalar_sem,
    hidden_sem,
    dout_sem,
    cross_send,
    cross_recv,
    first_send,
    first_hop,
    first_rest,
    second_send,
    second_hop,
    second_rest,
    third_send,
    third_recv,
    tally_send,
    tally_recv,
    result_sem,
    far,
):
    me = tuple(lax.axis_index(axis) for axis in AXES)
    core = me[3]

    def shifted(dim, by):
        return lax.rem(me[dim] + by, 4)

    def peer(dim, by):
        return tuple(shifted(dim, by) if axis == dim else me[axis] for axis in range(4))

    partner = (me[0], me[1], me[2], 1 - core)

    chunk = ROWS // HIDDEN_CHUNKS

    def hidden_copy(part):
        rows = pl.ds(part * chunk, chunk)
        return pltpu.make_async_copy(hidden_ref.at[rows], hidden_buf.at[rows], hidden_sem.at[part])

    def dout_copy(pair):
        slot = lax.rem(pair, DOUT_SLOTS)
        columns = pl.ds(pl.multiple_of(pair * PAIR, PAIR), PAIR)
        return pltpu.make_async_copy(dout_ref.at[:, columns], dout_buf.at[slot], dout_sem.at[slot])

    scalars = (
        pltpu.make_async_copy(counts_hbm, counts_ref, scalar_sem.at[0]),
        pltpu.make_async_copy(bucket_hbm, bucket_ref, scalar_sem.at[1]),
    )
    for copy in scalars:
        copy.start()
    hidden_copy(0).start()

    barrier = pltpu.get_barrier_semaphore()
    pl.semaphore_signal(barrier, inc=1, device_id=partner, device_id_type=MESH)
    for dim in range(3):
        for by in (1, 3):
            pl.semaphore_signal(barrier, inc=1, device_id=peer(dim, by), device_id_type=MESH)

    for part in range(1, HIDDEN_CHUNKS):
        hidden_copy(part).start()
    for pair in range(DOUT_SLOTS - 1):
        dout_copy(pair).start()

    for copy in scalars:
        copy.wait()
    own_count = counts_ref[0, bucket_ref[0]]

    for part in range(HIDDEN_CHUNKS):
        hidden_copy(part).wait()

        row = part * chunk
        position = lax.broadcasted_iota(jnp.int32, (chunk, 128), 0) + row
        live = jnp.where(position < own_count, 1.0, 0.0).astype(jnp.bfloat16)

        for unit in range(0, WIDTH, 128):
            masked = hidden_buf[pl.ds(row, chunk), pl.ds(unit, 128)] * live
            lhs[pl.ds(unit, 128), pl.ds(row, chunk)] = masked.T

    tally[0] = jnp.full((8, 128), own_count, jnp.int32).astype(jnp.float32)

    def remote(source, target, send, recv, device):
        return pltpu.make_async_remote_copy(
            src_ref=source,
            dst_ref=target,
            send_sem=send,
            recv_sem=recv,
            device_id=device,
            device_id_type=MESH,
        )

    def arrived(target, recv):
        remote(target, target, recv, recv, partner).wait_recv()

    def left(source, send):
        remote(source, source, send, send, partner).wait_send()

    def cross_copy(pair):
        slot = lax.rem(pair, THEIR_SLOTS)
        return remote(acc.at[slot], crossed.at[pair], cross_send.at[slot], cross_recv.at[pair], partner)

    def product(pair):
        slot = lax.rem(pair, DOUT_SLOTS)
        dout_copy(pair).wait()

        @pl.when(pair + (DOUT_SLOTS - 1) < PAIRS)
        def _():
            dout_copy(pair + (DOUT_SLOTS - 1)).start()

        theirs = lax.rem(pair, THEIR_SLOTS)
        mine = THEIR_SLOTS + pair
        place_0 = core * theirs + (1 - core) * mine
        place_1 = core * mine + (1 - core) * theirs
        for half in range(2):
            rows = pl.ds(half * (WIDTH // 2), WIDTH // 2)
            value = jnp.dot(lhs[rows, :], dout_buf[slot], preferred_element_type=jnp.float32)
            value = value.reshape(2, 4, 4, 2, 8, PAIR)
            acc[place_0, 2 * half : 2 * half + 2] = value[:, :, :, 0]
            acc[place_1, 2 * half : 2 * half + 2] = value[:, :, :, 1]

    def at(where):
        return tuple(where.get(dim, slice(None)) for dim in range(3))

    def half_of(side):
        return pl.ds(2 * side, 2)

    def first_region(order, place, side):
        cut = min(order[1], order[2])
        return at({order[0]: place, cut: half_of(side)})

    def second_region(order, place, side):
        return at({order[0]: me[order[0]], order[1]: place, order[2]: half_of(side)})

    def third_region(order, place):
        return at({order[0]: me[order[0]], order[1]: me[order[1]], order[2]: place})

    def gather(pair, size, region, terms):
        for step in range(size):
            spot = (THEIR_SLOTS + pair + step,) + region
            value = acc[spot]
            for ref, index in terms:
                value = value + ref[(pair + step,) + index]
            acc[spot] = value

    def first_copy(unit, kind):
        number, order, pair, size = unit
        by = (2, 2, 1, 3, 1, 3)[kind]
        side = (0, 1, 1, 0, 0, 1)[kind]
        region = first_region(order, shifted(order[0], by), side)
        recv = first_hop if kind < 2 else first_rest
        copy = remote(
            acc.at[(pl.ds(THEIR_SLOTS + pair, size),) + region],
            first_in.at[pl.ds(pair, size), kind],
            first_send,
            recv.at[number],
            peer(order[0], (1, 3)[kind % 2]),
        )
        return copy, region

    def second_copy(unit, kind):
        number, order, pair, size = unit
        by = (2, 2, 1, 3, 1, 3)[kind]
        side = (0, 1, 1, 0, 0, 1)[kind]
        region = second_region(order, shifted(order[1], by), side)
        recv = second_hop if kind < 2 else second_rest
        copy = remote(
            acc.at[(pl.ds(THEIR_SLOTS + pair, size),) + region],
            second_in.at[pl.ds(pair, size), kind],
            second_send,
            recv.at[number],
            peer(order[1], (1, 3)[kind % 2]),
        )
        return copy, region

    def direct_copy(unit, by, side):
        number, order, pair, size = unit
        region = second_region(order, shifted(order[1], by), side)
        return remote(
            acc.at[(pl.ds(THEIR_SLOTS + pair, size),) + region],
            second_in.at[pl.ds(pair, size), 2 * (by - 1) + side],
            second_send,
            second_rest.at[number],
            peer(order[1], by),
        )

    def third_copy(unit, by):
        number, order, pair, size = unit
        return remote(
            acc.at[(pl.ds(THEIR_SLOTS + pair, size),) + third_region(order, shifted(order[2], by))],
            third_in.at[pl.ds(THIRD_ORDER.index(number), size), by - 1],
            third_send,
            third_recv.at[THIRD_ORDER.index(number) // GROUP],
            peer(order[2], by),
        )

    def stage_1(unit):
        number, order, pair, size = unit
        for step in range(size):
            arrived(crossed.at[pair + step], cross_recv.at[pair + step])
        for kind in range(4):
            copy, region = first_copy(unit, kind)
            gather(pair, size, region, ((crossed, region),))
            copy.start()

    def stage_2(unit):
        number, order, pair, size = unit
        arrived(first_in.at[pl.ds(pair, size), pl.ds(0, 2)], first_hop.at[number])
        for kind in (4, 5):
            copy, region = first_copy(unit, kind)
            gather(pair, size, region, ((crossed, region), (first_in, (kind - 4,))))
            copy.start()

    def stage_3(unit):
        number, order, pair, size = unit
        arrived(first_in.at[pl.ds(pair, size), pl.ds(2, 4)], first_rest.at[number])
        for side, (up, down) in enumerate(((4, 3), (2, 5))):
            region = first_region(order, me[order[0]], side)
            gather(pair, size, region, ((crossed, region), (first_in, (up,)), (first_in, (down,))))
        if number in DIRECT:
            for by in (1, 2, 3):
                for side in range(2):
                    direct_copy(unit, by, side).start()
        else:
            for kind in range(4):
                second_copy(unit, kind)[0].start()

    def stage_4(unit):
        number, order, pair, size = unit
        arrived(second_in.at[pl.ds(pair, size), pl.ds(0, 2)], second_hop.at[number])
        for kind in (4, 5):
            copy, region = second_copy(unit, kind)
            gather(pair, size, region, ((second_in, (kind - 4,)),))
            copy.start()

    def stage_5(unit):
        number, order, pair, size = unit
        if number in DIRECT:
            arrived(second_in.at[pl.ds(pair, size)], second_rest.at[number])
        else:
            arrived(second_in.at[pl.ds(pair, size), pl.ds(2, 4)], second_rest.at[number])
        for side, (up, down) in enumerate(((4, 3), (2, 5))):
            region = second_region(order, me[order[1]], side)
            if number in DIRECT:
                gather(pair, size, region, tuple((second_in, (2 * by + side,)) for by in range(3)))
            else:
                gather(pair, size, region, ((second_in, (up,)), (second_in, (down,))))
        for by in (1, 2, 3):
            third_copy(unit, by).start()

    def result_copy(unit):
        number, order, pair, size = unit
        columns = pl.ds(pair * PAIR, size * PAIR)
        return pltpu.make_async_copy(result.at[:, columns], mean_ref.at[:, columns], result_sem)

    def stage_6(group):
        arrived(third_in.at[pl.ds(group * GROUP, GROUP)], third_recv.at[group])
        total = jnp.concatenate([tally[4]] * (PAIR // 128), axis=1)
        for rank in range(group * GROUP, (group + 1) * GROUP):
            unit = unit_of(THIRD_ORDER[rank])
            number, order, pair, size = unit
            value = acc[(THEIR_SLOTS + pair,) + third_region(order, me[order[2]])]
            for by in range(3):
                value = value + third_in[rank, by]
            result[:, pl.ds(pair * PAIR, PAIR)] = value / total
            result_copy(unit).start()

    def tally_start(level):
        if level == 0:
            remote(tally.at[0], tally_in.at[0, 0], tally_send.at[0], tally_recv.at[0], partner).start()
        else:
            for by in (1, 2, 3):
                remote(
                    tally.at[level],
                    tally_in.at[level, by - 1],
                    tally_send.at[level],
                    tally_recv.at[level],
                    peer(level - 1, by),
                ).start()

    def tally_end(level):
        number = 1 if level == 0 else 3
        arrived(tally_in.at[level, pl.ds(0, number)], tally_recv.at[level])
        left(tally_in.at[level, pl.ds(0, number)], tally_send.at[level])
        value = tally[level]
        for by in range(number):
            value = value + tally_in[level, by]
        tally[level + 1] = value

    def unit_of(number):
        return number, ORDERS[number], number, 1

    stages = (stage_1, stage_2, stage_3, stage_4, stage_5)

    def events(last):
        for event in EVENTS[last]:
            level, number = divmod(event, 100)
            if level == 6:
                stage_6(number)
            else:
                stages[level - 1](unit_of(number))

    product(0)
    pl.semaphore_wait(barrier, 7)
    for dim in range(3):
        pl.semaphore_signal(far, inc=1, device_id=peer(dim, 3), device_id_type=MESH)
    cross_copy(0).start()
    tally_start(0)
    for block in range(0, PAIRS, BLOCK):

        def step(pair, carry, block=block):

            @pl.when(pair >= THEIR_SLOTS)
            def _():
                left(acc.at[lax.rem(pair, THEIR_SLOTS)], cross_send.at[lax.rem(pair, THEIR_SLOTS)])

            product(pair)
            cross_copy(pair).start()
            for offset in range(BLOCK):
                last = block + offset
                if last + 1 < PAIRS:

                    @pl.when(pair == last)
                    def _(last=last):
                        events(last)
                        if last == TALLY_AFTER[0]:
                            pl.semaphore_wait(far, 3)
                        if last in TALLY_AFTER:
                            tally_end(TALLY_AFTER.index(last))
                            if last < TALLY_AFTER[-1]:
                                tally_start(TALLY_AFTER.index(last) + 1)

            return carry

        lax.fori_loop(max(block, 1), block + BLOCK, step, 0)
    events(PAIRS - 1)
    left(first_in, first_send)
    left(second_in, second_send)
    left(third_in, third_send)
    pltpu.make_async_copy(result, mean_ref, result_sem).wait()
    for slot in range(THEIR_SLOTS):
        left(acc.at[slot], cross_send.at[slot])


def reduced(counts, bucket_expert, hidden, dout):
    f32 = jnp.float32
    dma = pltpu.SemaphoreType.DMA
    away = pl.BlockSpec(memory_space=pl.ANY)
    return pl.pallas_call(
        kernel,
        out_shape=jax.ShapeDtypeStruct((8, PAIR * PAIRS), f32),
        in_specs=[away] * 4,
        out_specs=away,
        scratch_shapes=[
            pltpu.VMEM((ROWS, WIDTH), jnp.bfloat16),
            pltpu.VMEM((WIDTH, ROWS), jnp.bfloat16),
            pltpu.VMEM((DOUT_SLOTS, ROWS, PAIR), jnp.bfloat16),
            pltpu.VMEM((THEIR_SLOTS + PAIRS, 4, 4, 4, 8, PAIR), f32),
            pltpu.VMEM((PAIRS, 4, 4, 4, 8, PAIR), f32),
            pltpu.VMEM((PAIRS, 6, 2, 4, 8, PAIR), f32),
            pltpu.VMEM((PAIRS, 6, 2, 8, PAIR), f32),
            pltpu.VMEM((PAIRS, 3, 8, PAIR), f32),
            pltpu.VMEM((5, 8, 128), f32),
            pltpu.VMEM((4, 3, 8, 128), f32),
            pltpu.VMEM((8, PAIR * PAIRS), f32),
            pltpu.SMEM((1, 256), jnp.int32),
            pltpu.SMEM((1,), jnp.int32),
            dma((2,)),
            dma((HIDDEN_CHUNKS,)),
            dma((DOUT_SLOTS,)),
            dma((THEIR_SLOTS,)),
            dma((PAIRS,)),
            dma,
            dma((UNITS,)),
            dma((UNITS,)),
            dma,
            dma((UNITS,)),
            dma((UNITS,)),
            dma,
            dma((UNITS // GROUP,)),
            dma((4,)),
            dma((4,)),
            dma,
            pltpu.SemaphoreType.REGULAR,
        ],
        compiler_params=pltpu.CompilerParams(
            collective_id=0, has_side_effects=True, vmem_limit_bytes=67043328
        ),
    )(counts, bucket_expert, hidden, dout)


def body(hidden, dout, counts, bucket_expert, param, momentum):
    grad = reduced(counts, bucket_expert, hidden, dout)
    blend = first_beta * momentum + (1.0 - first_beta) * grad
    direction = jnp.tanh(blend / soft_width) + decay_rate * param
    new_param = param - learn_rate * direction
    new_momentum = second_beta * momentum + (1.0 - second_beta) * grad
    return (new_param, new_momentum, direction)


def solution(mesh):
    split = Mesh(mesh.devices.reshape(4, 4, 4, 2), AXES)
    rows = P(AXES, None)
    return jax.shard_map(
        body,
        mesh=split,
        in_specs=(rows, rows, rows, P(), rows, rows),
        out_specs=(rows, rows, rows),
        check_vma=False,
    )
```
